1024 devices in a mesh: blk: 8 (over y, core), uly: 4 (over x), dp: 32 (over z).
Axes of the slice: x: 4, y: 4, z: 32, core: 2. Of those that a mesh axis runs over, the one named last changes fastest.
Arguments:
- tokens: bfloat16 [8192, 4096], P(('uly', 'dp')), may hold values from -6 to 6
- expert_ids: int32 [8192, 8], P(('uly', 'dp')), may hold values from 0 to 127, all different within a row; in each aligned block of 64 rows (0 to 63, 64 to 127, ...) at most 5 rows name the same one
- route_weight: float32 [8192, 8], P(('uly', 'dp')), may hold values from 0.05 to 0.5
- w_gate: bfloat16 [128, 4096, 1024], P(('uly', 'dp'), None, 'blk'), may hold values from -0.09375 to 0.09375
- w_up: bfloat16 [128, 4096, 1024], P(('uly', 'dp'), None, 'blk'), may hold values from -0.09375 to 0.09375
- w_down: bfloat16 [128, 1024, 4096], P(('uly', 'dp'), 'blk'), may hold values from -0.1875 to 0.1875
Outputs:
- mixed: bfloat16 [8192, 4096], P(('uly', 'dp'), 'blk')
The draws below stay inside these ranges and needn't reach their ends.
Inputs may be any that keep to these rules, and one draw needn't show every extreme that they name: `expert_ids`: each row names 8 different experts. In each aligned block of 64 rows (the rows of one device) no expert is named by more than 5 rows, and in some block one expert is named by exactly 5 rows.
All inputs are finite; a program needn't handle non-finite values.
Results may differ from the reference program's by a relative error of at most 0.015.
Values may be sent and summed in bfloat16 or wider, within the bound.
No kernel may reach another device: no remote copies, remote signals or barrier semaphores. Data moves between devices by JAX's collectives and lax.ppermute only.
A program may use at most 32 MiB of HBM per device.

```python
import math
import jax
import jax.numpy as jnp
import numpy as np
from jax import lax

D = 4096
FF = 1024
TOPK = 8
TOK_DEV = 64
EXPERTS = 128
CAP = 5
TOKENS = 8192
N_BLK = 8
N_ULY = 4
N_DP = 32


def levels(own_key, shape, shards, least, largest):
    def one(axis_at, shards_of):
        heights = jax.random.uniform(jax.random.fold_in(jax.random.fold_in(own_key, 6), axis_at), (shards_of,), jnp.float32, least / len(shards), largest / len(shards))
        return jnp.repeat(jnp.exp(heights), shape[axis_at] // shards_of).reshape((-1,) + (1,) * (len(shape) - axis_at - 1))

    gain = one(*shards[0])
    for cut in shards[1:]:
        gain = gain * one(*cut)
    return gain


def shared_out(own_key, own, number, rows, number_of, top, limit, skew):
    ranking = jax.random.permutation(own_key, number_of)
    crowded, usual = load_shares(number_of, rows * top, limit, skew, True), load_shares(number_of, rows * top, limit, skew, False)
    places = jnp.arange(number_of)

    def named(tallies, turn):
        used = int((tallies > 0).sum())
        fixed = max(1, used // 4)
        moved = fixed + (places - fixed + turn * (used - fixed)) % max(1, number_of - fixed)
        return jnp.zeros((number_of,), jnp.int32).at[ranking[jnp.where(places < fixed, places, moved)]].set(jnp.asarray(tallies, jnp.int32))

    tallies = jnp.where(number % 4 == 0, named(crowded, number // 4), named(usual, number - number // 4 - 1))
    mixed = jax.random.permutation(jax.random.fold_in(own, 3), number_of)
    source_of, receiver = mixed[0:number_of // 2 * 2:2], mixed[1:number_of // 2 * 2:2]
    slack = jnp.minimum(tallies[source_of] - 1, limit - tallies[receiver]) // 2
    slack = jnp.where((source_of == ranking[0]) | (receiver == ranking[0]) | (tallies[receiver] == 0), 0, jnp.maximum(slack, 0))
    moved = jax.random.randint(jax.random.fold_in(own, 4), (number_of // 2,), 0, 1 << 20) % (slack + 1)
    tallies = tallies.at[source_of].add(-moved).at[receiver].add(moved)
    items = jnp.searchsorted(jnp.cumsum(tallies), jnp.arange(rows * top), side="right").astype(jnp.int32)
    table = items.reshape(top, rows).T
    table = table[jax.random.permutation(jax.random.fold_in(own, 1), rows)]
    turn = jax.random.randint(jax.random.fold_in(own, 2), (rows, 1), 0, top)
    return jnp.take_along_axis(table, (jnp.arange(top)[None, :] + turn) % top, axis=1)


def load_shares(count, total, most, skew, full):
    portions = [(1 << 20) // math.isqrt(grade ** skew) + 1 for grade in range(1, count + 1)]
    largest = most if full else min(most, max(-(-total // count), total * portions[0] // sum(portions)))
    least = 1 if total - largest >= count - 1 else 0
    given, rest = [largest] + [least] * (count - 1), total - largest - least * (count - 1)
    while rest > 0:
        candidates = [i for i in range(1, count) if given[i] < largest] or [i for i in range(1, count) if given[i] < most]
        whole, budget = sum([portions[i] for i in candidates]), rest
        for i in candidates:
            extra = min(most - given[i], max(1, budget * portions[i] // whole), rest)
            given[i] = given[i] + extra
            rest = rest - extra
    return np.array(given)


def scatter_about(stream_key, extent, deviation, most, cuts=(), held_as=jnp.bfloat16):
    array = deviation * jax.random.normal(stream_key, extent, jnp.float32)
    if cuts:
        array = array * levels(stream_key, extent, cuts, -0.22, 0.18)
    return jnp.clip(array, -most, most).astype(held_as)


def setup_inputs(seed: int = 0) -> dict:
    key_list = jax.random.split(jax.random.key(seed), 7)
    tokens = scatter_about(key_list[0], (TOKENS, D), 1.0, 6.0, ((0, 128),))
    expert_ids_keys = jax.random.split(jax.random.fold_in(key_list[1], 1), TOKENS // TOK_DEV)
    expert_ids_turns = jax.random.permutation(jax.random.fold_in(key_list[1], 3), TOKENS // TOK_DEV)
    expert_ids = jax.vmap(lambda own, number: shared_out(jax.random.fold_in(key_list[1], 2), own, number, TOK_DEV, EXPERTS, TOPK, CAP, 2))(expert_ids_keys, expert_ids_turns).reshape((TOKENS, TOPK))
    route_weight = jnp.clip(jnp.exp(math.log(0.5) - 2.3025851 * jax.random.uniform(key_list[2], (TOKENS, TOPK), jnp.float32) ** levels(key_list[2], (TOKENS, TOPK), ((0, 128),), -0.2, 0.2)), 0.05, 0.5)
    w_gate = scatter_about(key_list[3], (EXPERTS, D, FF), D ** -0.5, 0.09375, ((0, 128), (2, 8)))
    w_up = scatter_about(key_list[4], (EXPERTS, D, FF), D ** -0.5, 0.09375, ((0, 128), (2, 8)))
    w_down = scatter_about(key_list[5], (EXPERTS, FF, D), FF ** -0.5, 0.1875, ((0, 128), (1, 8)))
    return {"tokens": tokens, "expert_ids": expert_ids, "route_weight": route_weight, "w_gate": w_gate, "w_up": w_up, "w_down": w_down}


def reference(tokens, expert_ids, route_weight, w_gate, w_up, w_down):
    groups = N_ULY * N_DP
    model_width = tokens.shape[1]
    hidden_cut = FF // N_BLK
    grouped = tokens.reshape(groups, TOK_DEV, model_width)
    grouped_ids = expert_ids.reshape(groups, TOK_DEV, TOPK)
    weights = route_weight.reshape(groups, TOK_DEV, TOPK)
    labels = jnp.arange(EXPERTS, dtype=jnp.int32)
    onehot = (grouped_ids[:, :, :, None] == labels[None, None, None, :]).astype(jnp.int32)
    chosen = jnp.sum(onehot, axis=2)
    before = jnp.cumsum(chosen, axis=1) - chosen
    weight_share = jnp.sum(onehot.astype(route_weight.dtype) * weights[:, :, :, None], axis=2)
    positions = jnp.arange(TOK_DEV, dtype=jnp.int32)
    places = jnp.arange(CAP, dtype=jnp.int32)

    def one_expert(running, inputs):
        gate_matrix, up_matrix, down_matrix, picked, slot_rank, scaled = inputs
        matched = ((picked[:, :, None] == 1) & (slot_rank[:, :, None] == places[None, None, :])).astype(jnp.int32)
        source = jnp.sum(matched * positions[None, :, None], axis=1).astype(jnp.int32)
        filled = jnp.sum(matched, axis=1)
        index_full = jnp.broadcast_to(source[:, :, None], (groups, CAP, model_width)).astype(jnp.int32)
        selected = jnp.take_along_axis(grouped, index_full, axis=1)
        selected = jnp.where(filled[:, :, None] == 1, selected, jnp.zeros_like(selected))
        selected = selected.reshape(groups * CAP, model_width)
        gate_sum = jnp.dot(selected, gate_matrix, preferred_element_type=jnp.float32)
        up_sum = jnp.dot(selected, up_matrix, preferred_element_type=jnp.float32)
        hidden = (jax.nn.silu(gate_sum) * up_sum).astype(jnp.bfloat16)
        pieces = jnp.einsum("rbf,bfd->brd",
                            hidden.astype(jnp.float32).reshape(groups * CAP, N_BLK, hidden_cut),
                            down_matrix.astype(jnp.float32).reshape(N_BLK, hidden_cut, model_width))
        pieces = lax.optimization_barrier(pieces.astype(jnp.bfloat16)).astype(jnp.float32)
        answer = jnp.sum(pieces, axis=0).astype(jnp.bfloat16).reshape(groups, CAP, model_width)
        back_index = jnp.broadcast_to(jnp.clip(slot_rank, 0, CAP - 1)[:, :, None], (groups, TOK_DEV, model_width)).astype(jnp.int32)
        gathered = jnp.take_along_axis(answer, back_index, axis=1)
        return running + scaled[:, :, None] * gathered.astype(jnp.float32), None

    start_value = jnp.zeros((groups, TOK_DEV, model_width), jnp.float32)
    inputs = (w_gate, w_up, w_down,
              jnp.transpose(chosen, (2, 0, 1)),
              jnp.transpose(before, (2, 0, 1)),
              jnp.transpose(weight_share, (2, 0, 1)))
    running, _ = lax.scan(one_expert, start_value, inputs)
    return running.reshape(groups * TOK_DEV, model_width).astype(jnp.bfloat16)
```

```python
import jax
import jax.numpy as jnp
import numpy as np
from jax import lax
from jax.sharding import PartitionSpec as P

CAPACITY = 5
STEPS = 4
FORWARD = ((16, 9, 8, 1), (15, 10, 7, 2), (14, 11, 6, 3), (13, 12, 5, 4))
BACKWARD = ((15, 8, 7, 0), (14, 9, 6, 1), (13, 10, 5, 2), (12, 11, 4, 3))


def shift_table(n_blk, n_dp):
    rows = []
    for b in range(n_blk):
        if b % 2 == 0:
            rows.append([s for s in FORWARD[b // 2]])
        else:
            rows.append([(-s) % n_dp for s in BACKWARD[b // 2]])
    return np.array(rows, np.int32)


def move(value, shifts, step, sign, n_blk, n_dp):
    pairs = []
    for b in range(n_blk):
        s = sign * int(shifts[b, step])
        for z in range(n_dp):
            pairs.append((b * n_dp + z, b * n_dp + (z + s) % n_dp))
    return lax.ppermute(value, ("blk", "dp"), pairs)


def local(tokens, expert_ids, route_weight, w_gate, w_up, w_down):
    n_uly = lax.axis_size("uly")
    n_dp = lax.axis_size("dp")
    n_blk = lax.axis_size("blk")
    tokens_here, width = tokens.shape
    part = width // n_blk
    shifts = shift_table(n_blk, n_dp)
    b = lax.axis_index("blk")
    z = lax.axis_index("dp")

    w_down_full = lax.all_gather(w_down[0], "blk", axis=0, tiled=True)

    own_shifts = lax.dynamic_slice_in_dim(jnp.asarray(shifts), b, 1, 0)[0]
    z_of = (z + own_shifts) % n_dp
    experts = (jnp.arange(n_uly, dtype=jnp.int32)[:, None] * n_dp + z_of[None, :]).reshape(-1)
    hit = expert_ids[:, :, None] == experts[None, None, :]
    chosen = jnp.sum(hit.astype(jnp.float32), axis=1)
    weight = jnp.sum(jnp.where(hit, route_weight[:, :, None], 0.0), axis=1)
    row_i = lax.broadcasted_iota(jnp.int32, (tokens_here, tokens_here), 0)
    col_i = lax.broadcasted_iota(jnp.int32, (tokens_here, tokens_here), 1)
    earlier = (col_i < row_i).astype(jnp.float32)
    before = jnp.dot(earlier, chosen, preferred_element_type=jnp.float32)
    places = jnp.arange(CAPACITY, dtype=jnp.float32)
    at = (before.reshape(tokens_here, n_uly, 1, STEPS) == places[None, None, :, None]).astype(jnp.float32)
    placing = (at * chosen.reshape(tokens_here, n_uly, 1, STEPS)).astype(jnp.bfloat16)
    mixing = at * weight.reshape(tokens_here, n_uly, 1, STEPS)

    rows = n_uly * CAPACITY * STEPS
    outgoing = lax.dot_general(
        placing.reshape(tokens_here, rows), tokens, (((0,), (0,)), ((), ())), preferred_element_type=jnp.float32
    ).astype(jnp.bfloat16)
    outgoing = outgoing.reshape(n_uly, CAPACITY, STEPS, width)
    crossed = lax.all_to_all(outgoing, "uly", split_axis=0, concat_axis=0, tiled=True)
    arrived = []
    for j in range(STEPS):
        chunk = jnp.transpose(crossed[:, :, j, :], (1, 0, 2))
        arrived.append(move(chunk, shifts, j, 1, n_blk, n_dp))
    mine = jnp.stack(arrived).reshape(rows, width)
    mine, w_down_full = lax.optimization_barrier((mine, w_down_full))
    everyone = lax.all_gather(mine, "blk", axis=0, tiled=True)
    gate = jnp.dot(everyone, w_gate[0], preferred_element_type=jnp.float32)
    up = jnp.dot(everyone, w_up[0], preferred_element_type=jnp.float32)
    hidden = (jax.nn.silu(gate) * up).astype(jnp.bfloat16)
    hidden = hidden.reshape(n_blk, rows, hidden.shape[1])
    hidden = lax.all_to_all(hidden, "blk", split_axis=0, concat_axis=0, tiled=True)
    hidden = jnp.transpose(hidden, (1, 0, 2)).reshape(rows, -1)
    answer = jnp.dot(hidden, w_down_full, preferred_element_type=jnp.float32).astype(jnp.bfloat16)
    answer = answer.reshape(STEPS, CAPACITY, n_uly, width)
    back = [move(answer[j], shifts, j, -1, n_blk, n_dp) for j in range(STEPS)]
    back = jnp.transpose(jnp.stack(back), (2, 1, 0, 3))
    home = lax.all_to_all(back, "uly", split_axis=0, concat_axis=0, tiled=True).reshape(rows, width)
    mixed = jnp.dot(mixing.reshape(tokens_here, rows), home.astype(jnp.float32), precision=lax.Precision.HIGHEST)
    mixed = mixed.astype(jnp.bfloat16).reshape(tokens_here, n_blk, part)
    mixed = lax.all_to_all(jnp.transpose(mixed, (1, 0, 2)), "blk", split_axis=0, concat_axis=0, tiled=True)
    return jnp.sum(mixed.astype(jnp.float32), axis=0).astype(jnp.bfloat16)


def solution(mesh):
    return jax.shard_map(
        local,
        mesh=mesh,
        in_specs=(
            P(("uly", "dp"), None),
            P(("uly", "dp"), None),
            P(("uly", "dp"), None),
            P(("uly", "dp"), None, "blk"),
            P(("uly", "dp"), None, "blk"),
            P(("uly", "dp"), "blk", None),
        ),
        out_specs=P(("uly", "dp"), "blk"),
        check_vma=False,
    )
```

```python
import jax
import jax.numpy as jnp
import numpy as np
from jax import lax
from jax.sharding import PartitionSpec as P

CAPACITY = 5
STEPS = 4
DISTANCES = ((9, 8, 1), (15, 10, 7, 2), (14, 11, 6, 3), (13, 12, 5, 4))


def shift_table(n_blk, n_dp):
    half = n_dp // 2
    rows = []
    for b in range(n_blk):
        sign = 1 if b % 2 == 0 else -1
        steps = [(sign * s) % n_dp for s in DISTANCES[b // 2]]
        if b == 0:
            steps = [half] + steps
        if b == 1:
            steps = steps + [0]
        rows.append(steps)
    return np.array(rows, np.int32)


def move(value, shifts, step, sign, n_blk, n_dp):
    pairs = []
    for b in range(n_blk):
        s = sign * int(shifts[b, step])
        for z in range(n_dp):
            pairs.append((b * n_dp + z, b * n_dp + (z + s) % n_dp))
    return lax.ppermute(value, ("blk", "dp"), pairs)


def local(tokens, expert_ids, route_weight, w_gate, w_up, w_down):
    n_uly = lax.axis_size("uly")
    n_dp = lax.axis_size("dp")
    n_blk = lax.axis_size("blk")
    tokens_here, width = tokens.shape
    part = width // n_blk
    shifts = shift_table(n_blk, n_dp)
    b = lax.axis_index("blk")
    z = lax.axis_index("dp")

    w_down_full = lax.all_gather(w_down[0], "blk", axis=0, tiled=True)

    own_shifts = lax.dynamic_slice_in_dim(jnp.asarray(shifts), b, 1, 0)[0]
    z_of = (z + own_shifts) % n_dp
    experts = (jnp.arange(n_uly, dtype=jnp.int32)[:, None] * n_dp + z_of[None, :]).reshape(-1)
    hit = expert_ids[:, :, None] == experts[None, None, :]
    chosen = jnp.sum(hit.astype(jnp.float32), axis=1)
    weight = jnp.sum(jnp.where(hit, route_weight[:, :, None], 0.0), axis=1)
    row_i = lax.broadcasted_iota(jnp.int32, (tokens_here, tokens_here), 0)
    col_i = lax.broadcasted_iota(jnp.int32, (tokens_here, tokens_here), 1)
    earlier = (col_i < row_i).astype(jnp.float32)
    before = jnp.dot(earlier, chosen, preferred_element_type=jnp.float32)
    places = jnp.arange(CAPACITY, dtype=jnp.float32)
    at = (before.reshape(tokens_here, n_uly, 1, STEPS) == places[None, None, :, None]).astype(jnp.float32)
    placing = (at * chosen.reshape(tokens_here, n_uly, 1, STEPS)).astype(jnp.bfloat16)
    mixing = at * weight.reshape(tokens_here, n_uly, 1, STEPS)

    rows = n_uly * CAPACITY * STEPS
    outgoing = lax.dot_general(
        placing.reshape(tokens_here, rows), tokens, (((0,), (0,)), ((), ())), preferred_element_type=jnp.float32
    ).astype(jnp.bfloat16)
    outgoing = outgoing.reshape(n_uly, CAPACITY, STEPS, width)
    crossed = lax.all_to_all(outgoing, "uly", split_axis=0, concat_axis=0, tiled=True)
    arrived = []
    for j in range(STEPS):
        chunk = jnp.transpose(crossed[:, :, j, :], (1, 0, 2))
        arrived.append(move(chunk, shifts, j, 1, n_blk, n_dp))
    mine = jnp.stack(arrived).reshape(rows, width)
    mine, w_down_full = lax.optimization_barrier((mine, w_down_full))
    everyone = lax.all_gather(mine, "blk", axis=0, tiled=True)
    gate = jnp.dot(everyone, w_gate[0], preferred_element_type=jnp.float32)
    up = jnp.dot(everyone, w_up[0], preferred_element_type=jnp.float32)
    hidden = (jax.nn.silu(gate) * up).astype(jnp.bfloat16)
    hidden = hidden.reshape(n_blk, rows, hidden.shape[1])
    hidden = lax.all_to_all(hidden, "blk", split_axis=0, concat_axis=0, tiled=True)
    hidden = jnp.transpose(hidden, (1, 0, 2)).reshape(rows, -1)
    answer = jnp.dot(hidden, w_down_full, preferred_element_type=jnp.float32).astype(jnp.bfloat16)
    answer = answer.reshape(STEPS, CAPACITY, n_uly, width)
    back = [move(answer[j], shifts, j, -1, n_blk, n_dp) for j in range(STEPS)]
    back = jnp.transpose(jnp.stack(back), (2, 1, 0, 3))
    home = lax.all_to_all(back, "uly", split_axis=0, concat_axis=0, tiled=True).reshape(rows, width)
    mixed = jnp.dot(mixing.reshape(tokens_here, rows), home.astype(jnp.float32), precision=lax.Precision.HIGHEST)
    mixed = mixed.astype(jnp.bfloat16).reshape(tokens_here, n_blk, part)
    mixed = lax.all_to_all(jnp.transpose(mixed, (1, 0, 2)), "blk", split_axis=0, concat_axis=0, tiled=True)
    return jnp.sum(mixed.astype(jnp.float32), axis=0).astype(jnp.bfloat16)


def solution(mesh):
    return jax.shard_map(
        local,
        mesh=mesh,
        in_specs=(
            P(("uly", "dp"), None),
            P(("uly", "dp"), None),
            P(("uly", "dp"), None),
            P(("uly", "dp"), None, "blk"),
            P(("uly", "dp"), None, "blk"),
            P(("uly", "dp"), "blk", None),
        ),
        out_specs=P(("uly", "dp"), "blk"),
        check_vma=False,
    )
```

```python
import jax
import jax.numpy as jnp
import numpy as np
from jax import lax
from jax.sharding import PartitionSpec as P

CAPACITY = 5
DISTANCES = ((9, 8, 1), (15, 10, 7, 2), (14, 11, 6, 3), (13, 12, 5, 4))
CHUNKS = ((0, 3), (1, 2))
NEAR = (0, -1, 1, 2)


def shift_table(n_blk, n_dp):
    half = n_dp // 2
    rows = []
    for b in range(n_blk):
        sign = 1 if b % 2 == 0 else -1
        steps = [(sign * s) % n_dp for s in DISTANCES[b // 2]]
        if b == 0:
            steps = [half] + steps
        if b == 1:
            steps = steps + [0]
        rows.append(steps)
    return np.array(rows, np.int32)


def move(value, shifts, step, sign, n_blk, n_dp):
    pairs = []
    for b in range(n_blk):
        s = sign * int(shifts[b, step])
        for z in range(n_dp):
            pairs.append((b * n_dp + z, b * n_dp + (z + s) % n_dp))
    return lax.ppermute(value, ("blk", "dp"), pairs)


def chip_move(value, step, n_blk):
    chips = n_blk // 2
    return lax.ppermute(value, "blk", [(b, (b // 2 + step) % chips * 2 + b % 2) for b in range(n_blk)])


def core_swap(value, n_blk):
    return lax.ppermute(value, "blk", [(b, b ^ 1) for b in range(n_blk)])


def chip_gather(value, n_blk):
    half = value.shape[0] // 2
    below = chip_move(value, 1, n_blk)
    above = chip_move(value, -1, n_blk)
    far_low = chip_move(below[:half], 1, n_blk)
    far_high = chip_move(above[half:], -1, n_blk)
    own = jnp.concatenate([value, below, above, far_low, far_high], axis=0)
    return own, core_swap(own, n_blk)


def block(tokens, expert_ids, route_weight, w_gate, w_up, w_down):
    n_uly = lax.axis_size("uly")
    n_dp = lax.axis_size("dp")
    n_blk = lax.axis_size("blk")
    tokens_here, width = tokens.shape
    part = width // n_blk
    shifts = shift_table(n_blk, n_dp)
    b = lax.axis_index("blk")
    z = lax.axis_index("dp")

    down_own, down_other = chip_gather(w_down[0], n_blk)

    row_i = lax.broadcasted_iota(jnp.int32, (tokens_here, tokens_here), 0)
    col_i = lax.broadcasted_iota(jnp.int32, (tokens_here, tokens_here), 1)
    earlier = (col_i < row_i).astype(jnp.float32)
    places = jnp.arange(CAPACITY, dtype=jnp.float32)
    own_shifts = lax.dynamic_slice_in_dim(jnp.asarray(shifts), b, 1, 0)[0]
    order = [own_shifts[j] for steps in CHUNKS for j in steps]
    z_of = (z + jnp.stack(order)) % n_dp
    per = len(CHUNKS[0])
    rows = n_uly * CAPACITY * per
    x_of = jnp.arange(n_uly, dtype=jnp.int32) * n_dp
    experts = (x_of[None, :, None] + z_of.reshape(len(CHUNKS), 1, per)).reshape(-1)
    hit = expert_ids[:, :, None] == experts[None, None, :]
    chosen = jnp.sum(hit.astype(jnp.float32), axis=1)
    weight = jnp.sum(jnp.where(hit, route_weight[:, :, None], 0.0), axis=1)
    before = jnp.dot(earlier, chosen, preferred_element_type=jnp.float32)
    shape = (tokens_here, len(CHUNKS), n_uly, 1, per)
    at = (before.reshape(shape) == places[None, None, None, :, None]).astype(jnp.float32)
    placing = (at * chosen.reshape(shape)).astype(jnp.bfloat16).reshape(tokens_here, len(CHUNKS), rows)
    mixing = (at * weight.reshape(shape)).reshape(tokens_here, len(CHUNKS), rows)

    index_own = (b // 2 + jnp.array(NEAR, jnp.int32)) % (n_blk // 2) * 2 + b % 2
    index_other = index_own + 1 - 2 * (b % 2)

    outgoing = [
        lax.dot_general(placing[:, n], tokens, (((0,), (0,)), ((), ())), preferred_element_type=jnp.float32)
        .astype(jnp.bfloat16)
        .reshape(n_uly, CAPACITY, per, width)
        for n in range(len(CHUNKS))
    ]
    crossed = lax.all_to_all(jnp.stack(outgoing, axis=1), "uly", split_axis=0, concat_axis=0, tiled=True)
    gathered = []
    for n, steps in enumerate(CHUNKS):
        arrived = []
        for i, j in enumerate(steps):
            chunk = jnp.transpose(crossed[:, n, :, i, :], (1, 0, 2))
            arrived.append(move(chunk, shifts, j, 1, n_blk, n_dp))
        mine = jnp.stack(arrived).reshape(rows, n_blk, part)
        mine = jnp.transpose(mine, (1, 0, 2)).reshape(rows * n_blk, part)
        gathered.append(lax.all_gather(mine, "blk", axis=1, tiled=True))

    home = []
    answers = []
    for n, steps in enumerate(CHUNKS):
        everyone = gathered[n]
        if answers:
            everyone, _ = lax.optimization_barrier((everyone, answers[-1]))
        everyone = everyone.reshape(n_blk, rows, n_blk, part)
        everyone = jnp.transpose(everyone, (2, 1, 0, 3)).reshape(n_blk * rows, width)
        gate = jnp.dot(everyone, w_gate[0], preferred_element_type=jnp.float32)
        up = jnp.dot(everyone, w_up[0], preferred_element_type=jnp.float32)
        hidden = (jax.nn.silu(gate) * up).astype(jnp.bfloat16)
        units = hidden.shape[1]
        hidden = hidden.reshape(n_blk, rows, units)
        hidden = lax.all_to_all(hidden, "blk", split_axis=0, concat_axis=0, tiled=True)

        def pick(index):
            pieces = [lax.dynamic_index_in_dim(hidden, index[i], 0, keepdims=False) for i in range(len(NEAR))]
            return jnp.concatenate(pieces, axis=1)

        answer = jnp.dot(pick(index_own), down_own, preferred_element_type=jnp.float32)
        answer = answer + jnp.dot(pick(index_other), down_other, preferred_element_type=jnp.float32)
        answers.append(answer.astype(jnp.bfloat16).reshape(per, CAPACITY, n_uly, width))
    for n, steps in enumerate(CHUNKS):
        leaving = [answers[n][i] for i in range(per)]
        back = [move(leaving[i], shifts, j, -1, n_blk, n_dp) for i, j in enumerate(steps)]
        back = jnp.transpose(jnp.stack(back), (2, 1, 0, 3))
        home.append(lax.all_to_all(back, "uly", split_axis=0, concat_axis=0, tiled=True).reshape(rows, width))

    mixed = 0.0
    for n in range(len(CHUNKS)):
        mixed = mixed + jnp.dot(mixing[:, n], home[n].astype(jnp.float32), precision=lax.Precision.HIGHEST)
    mixed = mixed.astype(jnp.bfloat16).reshape(tokens_here, n_blk, part)
    mixed = lax.all_to_all(jnp.transpose(mixed, (1, 0, 2)), "blk", split_axis=0, concat_axis=0, tiled=True)
    return jnp.sum(mixed.astype(jnp.float32), axis=0).astype(jnp.bfloat16)


def solution(mesh):
    return jax.shard_map(
        block,
        mesh=mesh,
        in_specs=(
            P(("uly", "dp"), None),
            P(("uly", "dp"), None),
            P(("uly", "dp"), None),
            P(("uly", "dp"), None, "blk"),
            P(("uly", "dp"), None, "blk"),
            P(("uly", "dp"), "blk", None),
        ),
        out_specs=P(("uly", "dp"), "blk"),
        check_vma=False,
    )
```

```python
import jax
import jax.numpy as jnp
import numpy as np
from jax import lax
from jax.sharding import PartitionSpec as P

CAPACITY = 5
DISTANCES = ((9, 8, 1), (15, 10, 7, 2), (14, 11, 6, 3), (13, 12, 5, 4))
CHUNKS = ((0, 3), (1, 2))
NEAR = (0, -1, 1, 2)


def shift_table(n_blk, n_dp):
    half = n_dp // 2
    rows = []
    for b in range(n_blk):
        sign = 1 if b % 2 == 0 else -1
        steps = [(sign * s) % n_dp for s in DISTANCES[b // 2]]
        if b == 0:
            steps = [half] + steps
        if b == 1:
            steps = steps + [0]
        rows.append(steps)
    return np.array(rows, np.int32)


def move(value, shifts, step, sign, n_blk, n_dp):
    pairs = []
    for b in range(n_blk):
        s = sign * int(shifts[b, step])
        for z in range(n_dp):
            pairs.append((b * n_dp + z, b * n_dp + (z + s) % n_dp))
    return lax.ppermute(value, ("blk", "dp"), pairs)


def chip_move(value, step, n_blk):
    chips = n_blk // 2
    return lax.ppermute(value, "blk", [(b, (b // 2 + step) % chips * 2 + b % 2) for b in range(n_blk)])


def core_swap(value, n_blk):
    return lax.ppermute(value, "blk", [(b, b ^ 1) for b in range(n_blk)])


def chip_gather(value, n_blk):
    half = (value.shape[0] // 2 + 7) // 8 * 8
    below = chip_move(value, 1, n_blk)
    above = chip_move(value, -1, n_blk)
    far_low = chip_move(below[:half], 1, n_blk)
    far_high = chip_move(above[half:], -1, n_blk)
    own = jnp.concatenate([value, below, above, far_low, far_high], axis=0)
    return own, core_swap(own, n_blk)


def block(tokens, expert_ids, route_weight, w_gate, w_up, w_down):
    n_uly = lax.axis_size("uly")
    n_dp = lax.axis_size("dp")
    n_blk = lax.axis_size("blk")
    tokens_here, width = tokens.shape
    part = width // n_blk
    shifts = shift_table(n_blk, n_dp)
    b = lax.axis_index("blk")
    z = lax.axis_index("dp")

    down_own, down_other = chip_gather(w_down[0], n_blk)

    row_i = lax.broadcasted_iota(jnp.int32, (tokens_here, tokens_here), 0)
    col_i = lax.broadcasted_iota(jnp.int32, (tokens_here, tokens_here), 1)
    earlier = (col_i < row_i).astype(jnp.float32)
    places = jnp.arange(CAPACITY, dtype=jnp.float32)
    own_shifts = lax.dynamic_slice_in_dim(jnp.asarray(shifts), b, 1, 0)[0]
    order = [own_shifts[j] for steps in CHUNKS for j in steps]
    z_of = (z + jnp.stack(order)) % n_dp
    total = len(order)
    per = len(CHUNKS[0])
    rows = n_uly * CAPACITY * per
    experts = (jnp.arange(n_uly, dtype=jnp.int32)[:, None] * n_dp + z_of[None, :]).reshape(-1)
    hit = expert_ids[:, :, None] == experts[None, None, :]
    chosen = jnp.sum(hit.astype(jnp.float32), axis=1)
    weight = jnp.sum(jnp.where(hit, route_weight[:, :, None], 0.0), axis=1)
    before = jnp.dot(earlier, chosen, preferred_element_type=jnp.float32)
    shape = (tokens_here, n_uly, 1, total)
    at = (before.reshape(shape) == places[None, None, :, None]).astype(jnp.float32)
    placing = (at * chosen.reshape(shape)).astype(jnp.bfloat16).reshape(tokens_here, n_uly * CAPACITY * total)
    mixing = at * weight.reshape(shape)

    index_own = (b // 2 + jnp.array(NEAR, jnp.int32)) % (n_blk // 2) * 2 + b % 2
    index_other = index_own + 1 - 2 * (b % 2)

    near_of = jnp.array([0, 2, 3, 1], jnp.int32)
    chips = n_blk // 2
    to_all = jnp.arange(n_blk, dtype=jnp.int32)
    place_of = near_of[(to_all // 2 - b // 2) % chips] + chips * ((to_all + b) % 2)

    outgoing = lax.dot_general(
        placing, tokens, (((0,), (0,)), ((), ())), preferred_element_type=jnp.float32
    ).astype(jnp.bfloat16)
    crossed = lax.all_to_all(
        outgoing.reshape(n_uly, CAPACITY, total, width), "uly", split_axis=0, concat_axis=0, tiled=True
    )
    gathered = []
    for n, steps in enumerate(CHUNKS):
        arrived = []
        for i, j in enumerate(steps):
            chunk = jnp.transpose(crossed[:, :, n * per + i, :], (1, 0, 2))
            arrived.append(move(chunk, shifts, j, 1, n_blk, n_dp))
        mine = jnp.stack(arrived).reshape(rows, width)
        gathered.append(chip_gather(mine, n_blk))

    home = []
    answers = []
    for n, steps in enumerate(CHUNKS):
        halves = gathered[n]
        hidden = []
        for half in halves:
            gate = jnp.dot(half, w_gate[0], preferred_element_type=jnp.float32)
            up = jnp.dot(half, w_up[0], preferred_element_type=jnp.float32)
            hidden.append((jax.nn.silu(gate) * up).astype(jnp.bfloat16))
        units = hidden[0].shape[1]
        hidden = jnp.concatenate(hidden, axis=0).reshape(n_blk, rows, units)
        hidden = jnp.stack(
            [lax.dynamic_index_in_dim(hidden, place_of[i], 0, keepdims=False) for i in range(n_blk)]
        )
        hidden = lax.all_to_all(hidden, "blk", split_axis=0, concat_axis=0, tiled=True)

        def pick(index):
            pieces = [lax.dynamic_index_in_dim(hidden, index[i], 0, keepdims=False) for i in range(len(NEAR))]
            return jnp.concatenate(pieces, axis=1)

        answer = jnp.dot(pick(index_own), down_own, preferred_element_type=jnp.float32)
        answer = answer + jnp.dot(pick(index_other), down_other, preferred_element_type=jnp.float32)
        answers.append(answer.astype(jnp.bfloat16).reshape(per, CAPACITY, n_uly, width))
    for n, steps in enumerate(CHUNKS):
        leaving = [answers[n][i] for i in range(per)]
        back = [move(leaving[i], shifts, j, -1, n_blk, n_dp) for i, j in enumerate(steps)]
        back = jnp.transpose(jnp.stack(back), (2, 1, 0, 3))
        home.append(lax.all_to_all(back, "uly", split_axis=0, concat_axis=0, tiled=True).reshape(rows, width))

    mixed = 0.0
    for n in range(len(CHUNKS)):
        mixed = mixed + jnp.dot(mixing[:, :, :, n * per : (n + 1) * per].reshape(tokens_here, rows), home[n].astype(jnp.float32), precision=lax.Precision.HIGHEST)
    mixed = mixed.astype(jnp.bfloat16).reshape(tokens_here, n_blk, part)
    mixed = lax.all_to_all(jnp.transpose(mixed, (1, 0, 2)), "blk", split_axis=0, concat_axis=0, tiled=True)
    return jnp.sum(mixed.astype(jnp.float32), axis=0).astype(jnp.bfloat16)


def solution(mesh):
    return jax.shard_map(
        block,
        mesh=mesh,
        in_specs=(
            P(("uly", "dp"), None),
            P(("uly", "dp"), None),
            P(("uly", "dp"), None),
            P(("uly", "dp"), None, "blk"),
            P(("uly", "dp"), None, "blk"),
            P(("uly", "dp"), "blk", None),
        ),
        out_specs=P(("uly", "dp"), "blk"),
        check_vma=False,
    )
```

```python
import jax
import jax.numpy as jnp
import numpy as np
from jax import lax
from jax.experimental import pallas as pl
from jax.experimental.pallas import tpu as pltpu
from jax.sharding import PartitionSpec as P

CAPACITY = 5
STEPS = 4
DISTANCES = ((9, 8, 1), (15, 10, 7, 2), (14, 11, 6, 3), (13, 12, 5, 4))


def shift_table(n_blk, n_dp):
    half = n_dp // 2
    rows = []
    for b in range(n_blk):
        sign = 1 if b % 2 == 0 else -1
        steps = [(sign * s) % n_dp for s in DISTANCES[b // 2]]
        if b == 0:
            steps = [half] + steps
        if b == 1:
            steps = steps + [0]
        rows.append(steps)
    return np.array(rows, np.int32)


def move(value, shifts, step, sign, n_blk, n_dp):
    pairs = []
    for b in range(n_blk):
        s = sign * int(shifts[b, step])
        for z in range(n_dp):
            pairs.append((b * n_dp + z, b * n_dp + (z + s) % n_dp))
    return lax.ppermute(value, ("blk", "dp"), pairs)


def first_layer(blocks, w_gate, w_up, n_blk, rows):
    part = blocks.shape[1] // n_blk
    units = w_gate.shape[1]
    total = n_blk * rows

    def body(x_ref, gate_ref, up_ref, out_ref, sum_ref):
        step = pl.program_id(0)
        stacked = jnp.concatenate([x_ref[:, n * part : (n + 1) * part] for n in range(n_blk)], axis=0)
        both = jnp.concatenate([gate_ref[...], up_ref[...]], axis=1)
        product = jnp.dot(stacked, both, preferred_element_type=jnp.float32)

        @pl.when(step == 0)
        def _():
            sum_ref[...] = product

        @pl.when(step > 0)
        def _():
            sum_ref[...] += product

        @pl.when(step == n_blk - 1)
        def _():
            gate = sum_ref[:, :units]
            up = sum_ref[:, units:]
            out_ref[...] = (gate / (1.0 + jnp.exp(-gate)) * up).astype(jnp.bfloat16)

    return pl.pallas_call(
        body,
        grid=(n_blk,),
        in_specs=[
            pl.BlockSpec((rows, n_blk * part), lambda h: (h, 0)),
            pl.BlockSpec((part, units), lambda h: (h, 0)),
            pl.BlockSpec((part, units), lambda h: (h, 0)),
        ],
        out_specs=pl.BlockSpec((total, units), lambda h: (0, 0)),
        out_shape=jax.ShapeDtypeStruct((total, units), jnp.bfloat16),
        scratch_shapes=[pltpu.VMEM((total, 2 * units), jnp.float32)],
        compiler_params=pltpu.CompilerParams(dimension_semantics=("arbitrary",)),
        name="first_layer",
    )(blocks, w_gate, w_up)


def block(tokens, expert_ids, route_weight, w_gate, w_up, w_down):
    n_uly = lax.axis_size("uly")
    n_dp = lax.axis_size("dp")
    n_blk = lax.axis_size("blk")
    tokens_here, width = tokens.shape
    part = width // n_blk
    shifts = shift_table(n_blk, n_dp)
    b = lax.axis_index("blk")
    z = lax.axis_index("dp")

    w_down_full = lax.all_gather(w_down[0], "blk", axis=0, tiled=True)

    own_shifts = lax.dynamic_slice_in_dim(jnp.asarray(shifts), b, 1, 0)[0]
    z_of = (z + own_shifts) % n_dp
    experts = (jnp.arange(n_uly, dtype=jnp.int32)[:, None] * n_dp + z_of[None, :]).reshape(-1)
    hit = expert_ids[:, :, None] == experts[None, None, :]
    chosen = jnp.sum(hit.astype(jnp.float32), axis=1)
    weight = jnp.sum(jnp.where(hit, route_weight[:, :, None], 0.0), axis=1)
    row_i = lax.broadcasted_iota(jnp.int32, (tokens_here, tokens_here), 0)
    col_i = lax.broadcasted_iota(jnp.int32, (tokens_here, tokens_here), 1)
    earlier = (col_i < row_i).astype(jnp.float32)
    before = jnp.dot(earlier, chosen, preferred_element_type=jnp.float32)
    places = jnp.arange(CAPACITY, dtype=jnp.float32)
    at = (before.reshape(tokens_here, n_uly, 1, STEPS) == places[None, None, :, None]).astype(jnp.float32)
    placing = (at * chosen.reshape(tokens_here, n_uly, 1, STEPS)).astype(jnp.bfloat16)
    mixing = at * weight.reshape(tokens_here, n_uly, 1, STEPS)

    rows = n_uly * CAPACITY * STEPS
    outgoing = lax.dot_general(
        placing.reshape(tokens_here, rows), tokens, (((0,), (0,)), ((), ())), preferred_element_type=jnp.float32
    ).astype(jnp.bfloat16)
    outgoing = outgoing.reshape(n_uly, CAPACITY, STEPS, width)
    crossed = lax.all_to_all(outgoing, "uly", split_axis=0, concat_axis=0, tiled=True)
    arrived = []
    for j in range(STEPS):
        chunk = jnp.transpose(crossed[:, :, j, :], (1, 0, 2))
        arrived.append(move(chunk, shifts, j, 1, n_blk, n_dp))
    mine = jnp.stack(arrived).reshape(rows, n_blk, part)
    mine = jnp.transpose(mine, (1, 0, 2)).reshape(n_blk * rows, part)
    mine, w_down_full = lax.optimization_barrier((mine, w_down_full))
    everyone = lax.all_gather(mine, "blk", axis=1, tiled=True)
    hidden = first_layer(everyone, w_gate[0], w_up[0], n_blk, rows)
    hidden = hidden.reshape(n_blk, rows, hidden.shape[1])
    hidden = lax.all_to_all(hidden, "blk", split_axis=0, concat_axis=0, tiled=True)
    hidden = jnp.transpose(hidden, (1, 0, 2)).reshape(rows, -1)
    answer = jnp.dot(hidden, w_down_full, preferred_element_type=jnp.float32).astype(jnp.bfloat16)
    answer = answer.reshape(STEPS, CAPACITY, n_uly, width)
    back = []
    for j in range(STEPS):
        back.append(move(answer[j], shifts, j, -1, n_blk, n_dp))
    back = jnp.transpose(jnp.stack(back), (2, 1, 0, 3))
    home = lax.all_to_all(back, "uly", split_axis=0, concat_axis=0, tiled=True).reshape(rows, width)
    mixed = jnp.dot(mixing.reshape(tokens_here, rows), home.astype(jnp.float32), precision=lax.Precision.HIGHEST)
    mixed = mixed.astype(jnp.bfloat16).reshape(tokens_here, n_blk, part)
    mixed = lax.all_to_all(jnp.transpose(mixed, (1, 0, 2)), "blk", split_axis=0, concat_axis=0, tiled=True)
    return jnp.sum(mixed.astype(jnp.float32), axis=0).astype(jnp.bfloat16)


def solution(mesh):
    return jax.shard_map(
        block,
        mesh=mesh,
        in_specs=(
            P(("uly", "dp"), None),
            P(("uly", "dp"), None),
            P(("uly", "dp"), None),
            P(("uly", "dp"), None, "blk"),
            P(("uly", "dp"), None, "blk"),
            P(("uly", "dp"), "blk", None),
        ),
        out_specs=P(("uly", "dp"), "blk"),
        check_vma=False,
    )
```

```python
import jax
import jax.numpy as jnp
import numpy as np
from jax import lax
from jax.sharding import PartitionSpec as P

CAPACITY = 5
STEPS = 4
DISTANCES = ((9, 8, 1), (15, 10, 7, 2), (14, 11, 6, 3), (13, 12, 5, 4))


def shift_table(n_blk, n_dp):
    half = n_dp // 2
    rows = []
    for b in range(n_blk):
        sign = 1 if b % 2 == 0 else -1
        steps = [(sign * s) % n_dp for s in DISTANCES[b // 2]]
        if b == 0:
            steps = [half] + steps
        if b == 1:
            steps = steps + [0]
        rows.append(steps)
    return np.array(rows, np.int32)


def move(value, shifts, step, sign, n_blk, n_dp):
    pairs = []
    for b in range(n_blk):
        s = sign * int(shifts[b, step])
        for z in range(n_dp):
            pairs.append((b * n_dp + z, b * n_dp + (z + s) % n_dp))
    return lax.ppermute(value, ("blk", "dp"), pairs)


def local(tokens, expert_ids, route_weight, w_gate, w_up, w_down):
    n_uly = lax.axis_size("uly")
    n_dp = lax.axis_size("dp")
    n_blk = lax.axis_size("blk")
    tokens_here, width = tokens.shape
    part = width // n_blk
    shifts = shift_table(n_blk, n_dp)
    b = lax.axis_index("blk")
    z = lax.axis_index("dp")

    w_down_full = lax.all_gather(w_down[0], "blk", axis=0, tiled=True)

    same_core = [[2 * y + c for y in range(n_blk // 2)] for c in range(2)]

    def for_chip(weights):
        other = lax.ppermute(weights, "blk", [(n, n ^ 1) for n in range(n_blk)])
        first = lax.bitwise_and(b, 1) == 0
        low = jnp.where(first, weights, other)
        high = jnp.where(first, other, weights)
        return jnp.concatenate([low, high], axis=1)

    chip_gate = for_chip(w_gate[0])
    chip_up = for_chip(w_up[0])

    own_shifts = lax.dynamic_slice_in_dim(jnp.asarray(shifts), b, 1, 0)[0]
    z_of = (z + own_shifts) % n_dp
    experts = (jnp.arange(n_uly, dtype=jnp.int32)[:, None] * n_dp + z_of[None, :]).reshape(-1)
    hit = expert_ids[:, :, None] == experts[None, None, :]
    chosen = jnp.sum(hit.astype(jnp.float32), axis=1)
    weight = jnp.sum(jnp.where(hit, route_weight[:, :, None], 0.0), axis=1)
    row_i = lax.broadcasted_iota(jnp.int32, (tokens_here, tokens_here), 0)
    col_i = lax.broadcasted_iota(jnp.int32, (tokens_here, tokens_here), 1)
    earlier = (col_i < row_i).astype(jnp.float32)
    before = jnp.dot(earlier, chosen, preferred_element_type=jnp.float32)
    places = jnp.arange(CAPACITY, dtype=jnp.float32)
    at = (before.reshape(tokens_here, n_uly, 1, STEPS) == places[None, None, :, None]).astype(jnp.float32)
    placing = (at * chosen.reshape(tokens_here, n_uly, 1, STEPS)).astype(jnp.bfloat16)
    mixing = at * weight.reshape(tokens_here, n_uly, 1, STEPS)

    rows = n_uly * CAPACITY * STEPS
    outgoing = lax.dot_general(
        placing.reshape(tokens_here, rows), tokens, (((0,), (0,)), ((), ())), preferred_element_type=jnp.float32
    ).astype(jnp.bfloat16)
    outgoing = outgoing.reshape(n_uly, CAPACITY, STEPS, width)
    crossed = lax.all_to_all(outgoing, "uly", split_axis=0, concat_axis=0, tiled=True)
    arrived = []
    for j in range(STEPS):
        chunk = jnp.transpose(crossed[:, :, j, :], (1, 0, 2))
        arrived.append(move(chunk, shifts, j, 1, n_blk, n_dp))
    mine = jnp.stack(arrived).reshape(rows, width)
    mine, w_down_full = lax.optimization_barrier((mine, w_down_full))
    everyone = lax.all_gather(mine, "blk", axis=0, tiled=True, axis_index_groups=same_core)
    gate = jnp.dot(everyone, chip_gate, preferred_element_type=jnp.float32)
    up = jnp.dot(everyone, chip_up, preferred_element_type=jnp.float32)
    hidden = (jax.nn.silu(gate) * up).astype(jnp.bfloat16)
    hidden = hidden.reshape(n_blk // 2, rows, hidden.shape[1])
    hidden = lax.all_to_all(
        hidden, "blk", split_axis=0, concat_axis=0, tiled=True, axis_index_groups=same_core
    )
    hidden = jnp.transpose(hidden, (1, 0, 2)).reshape(rows, -1)
    answer = jnp.dot(hidden, w_down_full, preferred_element_type=jnp.float32).astype(jnp.bfloat16)
    answer = answer.reshape(STEPS, CAPACITY, n_uly, width)
    back = [move(answer[j], shifts, j, -1, n_blk, n_dp) for j in range(STEPS)]
    back = jnp.transpose(jnp.stack(back), (2, 1, 0, 3))
    home = lax.all_to_all(back, "uly", split_axis=0, concat_axis=0, tiled=True).reshape(rows, width)
    mixed = jnp.dot(mixing.reshape(tokens_here, rows), home.astype(jnp.float32), precision=lax.Precision.HIGHEST)
    mixed = mixed.astype(jnp.bfloat16).reshape(tokens_here, n_blk, part)
    mixed = lax.all_to_all(jnp.transpose(mixed, (1, 0, 2)), "blk", split_axis=0, concat_axis=0, tiled=True)
    return jnp.sum(mixed.astype(jnp.float32), axis=0).astype(jnp.bfloat16)


def solution(mesh):
    return jax.shard_map(
        local,
        mesh=mesh,
        in_specs=(
            P(("uly", "dp"), None),
            P(("uly", "dp"), None),
            P(("uly", "dp"), None),
            P(("uly", "dp"), None, "blk"),
            P(("uly", "dp"), None, "blk"),
            P(("uly", "dp"), "blk", None),
        ),
        out_specs=P(("uly", "dp"), "blk"),
        check_vma=False,
    )
```

```python
import jax
import jax.numpy as jnp
import numpy as np
from jax import lax
from jax.sharding import PartitionSpec as P

CAPACITY = 5
STEPS = 4
DISTANCES = ((13, 9, 2), (15, 12, 4, 1), (14, 10, 5, 3), (11, 8, 7, 6))


def shift_table(n_blk, n_dp):
    half = n_dp // 2
    rows = []
    for b in range(n_blk):
        sign = 1 if b % 2 == 0 else -1
        steps = [(sign * s) % n_dp for s in DISTANCES[b // 2]]
        if b == 0:
            steps = [half] + steps
        if b == 1:
            steps = steps + [0]
        rows.append(steps)
    return np.array(rows, np.int32)


def move(value, shifts, step, sign, n_blk, n_dp):
    pairs = []
    for b in range(n_blk):
        s = sign * int(shifts[b, step])
        for z in range(n_dp):
            pairs.append((b * n_dp + z, b * n_dp + (z + s) % n_dp))
    return lax.ppermute(value, ("blk", "dp"), pairs)


def block(tokens, expert_ids, route_weight, w_gate, w_up, w_down):
    n_uly = lax.axis_size("uly")
    n_dp = lax.axis_size("dp")
    n_blk = lax.axis_size("blk")
    tokens_here, width = tokens.shape
    part = width // n_blk
    shifts = shift_table(n_blk, n_dp)
    b = lax.axis_index("blk")
    z = lax.axis_index("dp")

    w_down_full = lax.all_gather(w_down[0], "blk", axis=0, tiled=True)

    same_core = [[2 * y + c for y in range(n_blk // 2)] for c in range(2)]

    def for_chip(weights):
        other = lax.ppermute(weights, "blk", [(n, n ^ 1) for n in range(n_blk)])
        first = lax.bitwise_and(b, 1) == 0
        low = jnp.where(first, weights, other)
        high = jnp.where(first, other, weights)
        return jnp.concatenate([low, high], axis=1)

    chip_gate = for_chip(w_gate[0])
    chip_up = for_chip(w_up[0])

    own_shifts = lax.dynamic_slice_in_dim(jnp.asarray(shifts), b, 1, 0)[0]
    z_of = (z + own_shifts) % n_dp
    experts = (jnp.arange(n_uly, dtype=jnp.int32)[:, None] * n_dp + z_of[None, :]).reshape(-1)
    hit = expert_ids[:, :, None] == experts[None, None, :]
    chosen = jnp.sum(hit.astype(jnp.float32), axis=1)
    weight = jnp.sum(jnp.where(hit, route_weight[:, :, None], 0.0), axis=1)
    row_i = lax.broadcasted_iota(jnp.int32, (tokens_here, tokens_here), 0)
    col_i = lax.broadcasted_iota(jnp.int32, (tokens_here, tokens_here), 1)
    earlier = (col_i < row_i).astype(jnp.float32)
    before = jnp.dot(earlier, chosen, preferred_element_type=jnp.float32)
    places = jnp.arange(CAPACITY, dtype=jnp.float32)
    at = (before.reshape(tokens_here, n_uly, 1, STEPS) == places[None, None, :, None]).astype(jnp.float32)
    placing = (at * chosen.reshape(tokens_here, n_uly, 1, STEPS)).astype(jnp.bfloat16)
    mixing = at * weight.reshape(tokens_here, n_uly, 1, STEPS)

    rows = n_uly * CAPACITY * STEPS
    outgoing = lax.dot_general(
        placing.reshape(tokens_here, rows), tokens, (((0,), (0,)), ((), ())), preferred_element_type=jnp.float32
    ).astype(jnp.bfloat16)
    outgoing = outgoing.reshape(n_uly, CAPACITY, STEPS, width)
    crossed = lax.all_to_all(outgoing, "uly", split_axis=0, concat_axis=0, tiled=True)
    arrived = []
    for j in range(STEPS):
        chunk = jnp.transpose(crossed[:, :, j, :], (1, 0, 2))
        arrived.append(move(chunk, shifts, j, 1, n_blk, n_dp))
    mine = jnp.stack(arrived).reshape(rows, width)
    mine, w_down_full = lax.optimization_barrier((mine, w_down_full))
    everyone = lax.all_gather(mine, "blk", axis=0, tiled=True, axis_index_groups=same_core)
    gate = jnp.dot(everyone, chip_gate, preferred_element_type=jnp.float32)
    up = jnp.dot(everyone, chip_up, preferred_element_type=jnp.float32)
    hidden = (jax.nn.silu(gate) * up).astype(jnp.bfloat16)
    hidden = hidden.reshape(n_blk // 2, rows, hidden.shape[1])
    hidden = lax.all_to_all(
        hidden, "blk", split_axis=0, concat_axis=0, tiled=True, axis_index_groups=same_core
    )
    hidden = jnp.transpose(hidden, (1, 0, 2)).reshape(rows, -1)
    answer = jnp.dot(hidden, w_down_full, preferred_element_type=jnp.float32).astype(jnp.bfloat16)
    answer = answer.reshape(STEPS, CAPACITY, n_uly, width)
    back = []
    for j in range(STEPS):
        back.append(move(answer[j], shifts, j, -1, n_blk, n_dp))
    back = jnp.transpose(jnp.stack(back), (2, 1, 0, 3))
    home = lax.all_to_all(back, "uly", split_axis=0, concat_axis=0, tiled=True).reshape(rows, width)
    mixed = jnp.dot(mixing.reshape(tokens_here, rows), home.astype(jnp.float32), precision=lax.Precision.HIGHEST)
    mixed = mixed.astype(jnp.bfloat16).reshape(tokens_here, n_blk, part)
    mixed = lax.all_to_all(jnp.transpose(mixed, (1, 0, 2)), "blk", split_axis=0, concat_axis=0, tiled=True)
    return jnp.sum(mixed.astype(jnp.float32), axis=0).astype(jnp.bfloat16)


def solution(mesh):
    return jax.shard_map(
        block,
        mesh=mesh,
        in_specs=(
            P(("uly", "dp"), None),
            P(("uly", "dp"), None),
            P(("uly", "dp"), None),
            P(("uly", "dp"), None, "blk"),
            P(("uly", "dp"), None, "blk"),
            P(("uly", "dp"), "blk", None),
        ),
        out_specs=P(("uly", "dp"), "blk"),
        check_vma=False,
    )
```
